128 devices in a mesh: group: 4 (over x_lo, core), shard: 32 (over z, y, x_hi).
Axes of the slice: x: 4 (x_hi: 2, x_lo: 2; x = x_hi * 2 + x_lo), y: 4, z: 4, core: 2. Of those that a mesh axis runs over, the one named last changes fastest.
Arguments:
- step_index: int32 [1], replicated, may hold values from 0 to 1023
- hidden: bfloat16 [4, 32768, 4608], P('group', 'shard'), may hold values from -600 to 600
- upstream: bfloat16 [4, 32768, 2304], P('group', 'shard'), may hold values from -40 to 40
- numerator: float32 [4, 4608, 2304], P('group', 'shard'), may hold values from -6 to 6
- push_weight: float32 [4], P('group'), may hold values from 0.5 to 2
Outputs:
- numerator_next: float32 [4, 4608, 2304], P('group', 'shard')
- weight_next: float32 [4], P('group')
- params: bfloat16 [4, 4608, 2304], P('group', 'shard')
The draws below stay inside these ranges and needn't reach their ends.
All inputs are finite; a program needn't handle non-finite values.
Results may differ from the reference program's by a relative error of at most 0.009.
Values may be sent and summed in bfloat16 or wider, within the bound.
A program may use at most 128 MiB of HBM per device.

```python
import math
import jax
import jax.numpy as jnp
from jax import lax

D = 2304
FF = 4608
TOK_DEV = 1024
GROUPS = 4
SHARDS = 32
TOK_GROUP = 32768


def draw_hidden(key, part):
    keys = jax.random.split(key, 4)
    position = jnp.arange(FF, dtype=jnp.float32)
    column_scale = 10.0 ** jax.random.uniform(keys[0], (FF,), jnp.float32) * 3.0 ** (position / FF) / 4.0
    row_scale = 10.0 ** jax.random.uniform(keys[1], (GROUPS, TOK_GROUP, 1), jnp.float32) / 4.0
    owner = jax.random.permutation(keys[2], SHARDS)
    token_block = jnp.arange(TOK_GROUP) // TOK_DEV
    unit_block = jnp.arange(FF) // (FF // SHARDS)
    spike = jnp.where(owner[token_block][:, None] == unit_block[None, :], 3.0, 1.0)
    shape = (GROUPS, TOK_GROUP, FF)
    base = jnp.clip(jax.random.normal(keys[3], shape, jnp.float32), -5.0, 5.0)
    return (base * row_scale * column_scale * spike).astype(jnp.bfloat16)


def draw_upstream(key, part):
    keys = jax.random.split(key, 2)
    column_scale = 10.0 ** jax.random.uniform(keys[0], (D,), jnp.float32) / 3.0
    shape = (GROUPS, TOK_GROUP, D)
    base = jnp.clip(jax.random.normal(keys[1], shape, jnp.float32), -5.0, 5.0)
    return (base * column_scale).astype(jnp.bfloat16)


def steps_of(stream_key, shape, shards, smallest, high):
    gain, own = 1.0, jax.random.fold_in(stream_key, 6)
    for axis_at, parts in shards:
        heights = jnp.exp(jax.random.uniform(jax.random.fold_in(own, axis_at), (parts,), jnp.float32, smallest / len(shards), high / len(shards)))
        gain = gain * jnp.repeat(heights, shape[axis_at] // parts).reshape([-1 if axis == axis_at else 1 for axis in range(len(shape))])
    return gain


def scatter_about(own_key, dims, scale, bound, cuts=(), held_as=jnp.bfloat16):
    level = steps_of(own_key, dims, cuts, -0.22, 0.18) if cuts else 1.0
    result = jax.random.normal(own_key, dims, jnp.float32) * scale * level
    return jnp.minimum(jnp.maximum(result, -bound), bound).astype(held_as)


def setup_inputs(seed: int = 0) -> dict:
    splits = jax.random.split(jax.random.key(seed), 6)
    return {
        "step_index": jax.random.randint(splits[0], (1,), 0, 1024).astype(jnp.int32),
        "hidden": draw_hidden(jax.random.fold_in(splits[5], 71), 0),
        "upstream": draw_upstream(jax.random.fold_in(splits[5], 71), 0),
        "numerator": scatter_about(splits[3], (GROUPS, FF, D), 1.0, 6.0, ((0, 4), (1, 32)), jnp.float32),
        "push_weight": jnp.clip(jnp.exp(math.log(2.0) - 1.3862944 * jax.random.uniform(splits[4], (GROUPS,), jnp.float32) ** steps_of(splits[4], (GROUPS,), ((0, 4),), -0.2, 0.2)), 0.5, 2.0),
    }


learning_rate = 0.3
decay_steps = 256.0
clip_ceiling = 1.0
epsilon = 1e-06

def shard_gradient(hidden_rows, upstream_rows):
    hidden_blocks = hidden_rows.reshape(SHARDS, TOK_DEV, FF)
    upstream_blocks = upstream_rows.reshape(SHARDS, TOK_DEV, D)

    def accumulate(running, shard_pair):
        product = jnp.dot(shard_pair[0].astype(jnp.float32).T, shard_pair[1].astype(jnp.float32), preferred_element_type=jnp.float32, precision=lax.Precision.HIGHEST)
        rounded = lax.optimization_barrier(product.astype(jnp.bfloat16))
        return (running + rounded.astype(jnp.float32), None)
    summed, unused = lax.scan(accumulate, jnp.zeros((FF, D), jnp.float32), (hidden_blocks, upstream_blocks))
    return summed

def group_pair(arrays):
    return shard_gradient(arrays[0], arrays[1])

def reference(step_index, hidden, upstream, numerator, push_weight):
    gradient = lax.map(group_pair, (hidden, upstream))
    square_mean = lax.optimization_barrier(jnp.sum(gradient * gradient, axis=(1, 2))) / (FF * D)
    rate = learning_rate / jnp.sqrt(1.0 + step_index[0].astype(jnp.float32) / decay_steps)
    factor = rate * jnp.minimum(1.0, clip_ceiling / jnp.sqrt(square_mean + epsilon))
    pushed = numerator - factor[:, None, None] * gradient
    level_count = GROUPS.bit_length() - 1
    exponent = (step_index[0] % level_count).astype(jnp.int32)
    offset = jnp.left_shift(jnp.int32(1), exponent)
    peer_state = jnp.roll(pushed, offset, axis=0)
    peer_weight = jnp.roll(push_weight, offset, axis=0)
    numerator_next = 0.5 * (pushed + peer_state)
    weight_next = 0.5 * (push_weight + peer_weight)
    params = (numerator_next / weight_next[:, None, None]).astype(jnp.bfloat16)
    return (numerator_next, weight_next, params)
```

```python
import functools

import jax
import jax.numpy as jnp
from jax import lax
from jax.experimental import pallas as pl
from jax.experimental.pallas import tpu as pltpu
from jax.sharding import PartitionSpec as P

learning_rate = 0.3
decay_steps = 256.0
clip_ceiling = 1.0
epsilon = 1e-06

MESH = pl.DeviceIdType.MESH
RING = 4
LANES = 128
f32 = jnp.float32
bf16 = jnp.bfloat16


def kernel(
    entry_count,
    step_ref, weight_ref, hidden_hbm, upstream_hbm, numerator_hbm,
    gradient_out, peer_gradient_out, peer_numerator_out, coefficients_out,
    hidden, upstream, numerator, numerator_short, part, transit, final, across, last,
    gradient, gradient_short, squares, norms, meta,
    load_sem, out_sem, transit_send, transit_recv, final_send, final_recv,
    across_send, across_recv, last_send, last_recv, gossip_send, gossip_recv,
    state_send, state_recv, norm_send, norm_recv, meta_send, meta_recv,
):
    steps = part.shape[0]
    rows = part.shape[5]
    quarter = hidden.shape[1] // RING
    group = lax.axis_index("group")
    shard = lax.axis_index("shard")
    groups = lax.axis_size("group")
    shards = lax.axis_size("shard")
    z = shard // (2 * RING)
    y = (shard // 2) % RING
    xh = shard % 2

    def place(kind, first, second, half):
        zz, yy = (first, second) if kind == 0 else (second, first)
        return (group, zz * (2 * RING) + yy * 2 + half)

    def send(src, dst, send_sem, recv_sem, device):
        pltpu.make_async_remote_copy(
            src_ref=src, dst_ref=dst, send_sem=send_sem, recv_sem=recv_sem,
            device_id=device, device_id_type=MESH,
        ).start()

    def arrived(ref, sem):
        pltpu.make_async_copy(ref, ref, sem).wait()

    own = ((z, y), (y, z))

    def hidden_columns(i):
        block = (z + (2, 1, 3, 0)[i]) % RING if isinstance(i, int) else None
        return pl.ds(pl.multiple_of(block * quarter, LANES), quarter)

    wide = 2 * LANES
    loads = []
    loads.append(pltpu.make_async_copy(upstream_hbm.at[:, 0:wide], upstream.at[:, 0:wide], load_sem.at[4]))
    for i in range(RING):
        loads.append(pltpu.make_async_copy(
            hidden_hbm.at[:, hidden_columns(i)], hidden.at[:, hidden_columns(i)], load_sem.at[i]))
    loads.append(pltpu.make_async_copy(upstream_hbm.at[:, wide:], upstream.at[:, wide:], load_sem.at[5]))
    loads.append(pltpu.make_async_copy(numerator_hbm, numerator, load_sem.at[6]))
    for load in loads:
        load.start()

    barrier = pltpu.get_barrier_semaphore()
    partners = [(group, place(0, (z + k) % RING, y, xh)[1]) for k in range(1, RING)]
    partners += [(group, place(0, z, (y + k) % RING, xh)[1]) for k in range(1, RING)]
    partners += [(group, place(0, z, y, 1 - xh)[1])]
    partners += [((group + k) % groups, shard) for k in range(1, RING)]
    for device in partners:
        pl.semaphore_signal(barrier, inc=1, device_id=device, device_id_type=MESH)
    squares[...] = jnp.zeros_like(squares)
    loads[0].wait()

    def sum_of(*refs):
        total = refs[0][...].astype(f32)
        for ref in refs[1:]:
            total = total + ref[...].astype(f32)
        return total

    def open_step(t):
        columns = pl.ds(pl.multiple_of(t * wide, wide), wide)

        @pl.when(t == 1)
        def _():
            loads[5].wait()

        def block(i, carry):
            distance = jnp.where(i == 0, 2, jnp.where(i == 1, 1, jnp.where(i == 2, 3, 0)))
            to = (z + distance) % RING

            for j in range(RING):
                @pl.when((t == 0) & (i == j))
                def _(j=j):
                    loads[1 + j].wait()

            product = lax.dot_general(
                hidden[:, pl.ds(pl.multiple_of(to * quarter, LANES), quarter)],
                upstream[:, columns],
                (((0,), (0,)), ((), ())),
                preferred_element_type=f32,
            )
            for b in range(RING):
                for h in range(2):
                    at = (b * 2 + h) * rows
                    part[t, 0, to, h, b] = product[at:at + rows, :LANES].astype(bf16)
                    part[t, 1, b, h, to] = product[at:at + rows, LANES:].astype(bf16)

            @pl.when((t == 0) & (i == 0))
            def _():
                pl.semaphore_wait(barrier, len(partners))

            @pl.when(i == 0)
            def _():
                first_sends(t, 0)

            @pl.when(i == 1)
            def _():
                direct_send(t, 0, 1)

            @pl.when(i == 2)
            def _():
                direct_send(t, 0, 3)

            return carry

        lax.fori_loop(0, RING, block, 0)
        first_sends(t, 1)
        direct_send(t, 1, 1)
        direct_send(t, 1, 3)

    def first_sends(t, kind):
        a, b = own[kind]
        to = (a + 2) % RING
        for h, hop in ((0, 3), (1, 1)):
            send(part.at[t, kind, to, h], transit.at[t, kind, h], transit_send.at[t],
                 transit_recv.at[t, kind, h], place(kind, (a + hop) % RING, b, xh))

    def direct_send(t, kind, hop):
        a, b = own[kind]
        to = (a + hop) % RING
        h = 0 if hop == 1 else 1
        send(part.at[t, kind, to, h], final.at[t, kind, h], final_send.at[t],
             final_recv.at[t, kind], place(kind, to, b, xh))

    def relay_step(t):
        for kind in range(2):
            a, b = own[kind]
            for h, hop in ((0, 3), (1, 1)):
                to = (a + hop) % RING
                arrived(transit.at[t, kind, h], transit_recv.at[t, kind, h])
                part[t, kind, to, h] = sum_of(part.at[t, kind, to, h], transit.at[t, kind, h]).astype(bf16)
                send(part.at[t, kind, to, h], final.at[t, kind, 2 + h], final_send.at[t],
                     final_recv.at[t, kind], place(kind, to, b, xh))

    def across_step(t):
        for kind in range(2):
            a, b = own[kind]
            arrived(final.at[t, kind], final_recv.at[t, kind])
            for h in range(2):
                part[t, kind, a, h] = sum_of(
                    part.at[t, kind, a, h], final.at[t, kind, h], final.at[t, kind, 2 + h]).astype(bf16)
            send(part.at[t, kind, a, 1 - xh], across.at[t, kind], across_send.at[t],
                 across_recv.at[t, kind], place(kind, a, b, 1 - xh))

    def last_step(t):
        for kind in range(2):
            a, b = own[kind]
            arrived(across.at[t, kind], across_recv.at[t, kind])
            part[t, kind, a, xh] = sum_of(part.at[t, kind, a, xh], across.at[t, kind]).astype(bf16)
            for hop in (2, 1, 3):
                to = (b + hop) % RING
                send(part.at[t, kind, a, xh, to], last.at[t, kind, hop - 1], last_send.at[t],
                     last_recv.at[t, kind], place(kind, a, to, xh))

    def close_step(t):
        for kind in range(2):
            a, b = own[kind]
            arrived(last.at[t, kind], last_recv.at[t, kind])
            total = sum_of(part.at[t, kind, a, xh, b], last.at[t, kind, 0], last.at[t, kind, 1], last.at[t, kind, 2])
            at = slice(kind * LANES, (kind + 1) * LANES)
            gradient[t, :, at] = total
            gradient_short[t, :, at] = total.astype(bf16)
            squares[...] += jnp.sum((total * total).reshape(rows // 8, 8, LANES), axis=0)
        columns = pl.ds(pl.multiple_of(t * wide, wide), wide)
        for k in (1, 2):
            send(gradient_short.at[t], peer_gradient_out.at[k - 1, :, columns], gossip_send.at[t],
                 gossip_recv.at[k - 1], ((group + k) % groups, shard))
        pltpu.make_async_copy(gradient.at[t], gradient_out.at[:, columns], out_sem.at[t]).start()

    def turn(t, carry):
        @pl.when(t < steps)
        def _():
            open_step(t)

        @pl.when((t >= 1) & (t < steps + 1))
        def _():
            relay_step(t - 1)

        @pl.when(t == 0)
        def _():
            loads[6].wait()
            numerator_short[...] = numerator[...].astype(bf16)

        @pl.when(t == 1)
        def _():
            for k in (1, 2):
                send(numerator_short, peer_numerator_out.at[k - 1], state_send.at[k - 1],
                     state_recv.at[k - 1], ((group + k) % groups, shard))

        @pl.when((t >= 2) & (t < steps + 2))
        def _():
            across_step(t - 2)

        @pl.when((t >= 3) & (t < steps + 3))
        def _():
            last_step(t - 3)

        @pl.when(t >= 4)
        def _():
            close_step(t - 4)

        return carry

    lax.fori_loop(0, steps + 4, turn, 0)

    norms[0:1] = jnp.sum(squares[...], axis=0, keepdims=True)

    def tell(k, carry):
        send(norms.at[0:1], norms.at[pl.ds(k, 1)], norm_send.at[0], norm_recv.at[0], (group, (shard + k) % shards))
        return carry

    lax.fori_loop(1, shards, tell, 0)
    arrived(norms.at[1:shards], norm_recv.at[0])
    square_sum = jnp.sum(norms[...], keepdims=True)
    first_row = lax.broadcasted_iota(jnp.int32, (8, LANES), 0) == 0
    own_weight = jnp.full((8, LANES), weight_ref[0], f32)
    meta[0] = jnp.where(first_row, square_sum, own_weight)
    for k in (1, 2):
        send(meta.at[0], meta.at[k], meta_send.at[k - 1], meta_recv.at[k - 1], ((group + k) % groups, shard))

    arrived(norms.at[1:shards], norm_send.at[0])
    def drain(t, carry):
        arrived(transit.at[t], transit_send.at[t])
        arrived(final.at[t], final_send.at[t])
        arrived(across.at[t], across_send.at[t])
        arrived(last.at[t], last_send.at[t])
        pltpu.make_async_copy(gradient.at[t], gradient_out.at[:, 0:wide], out_sem.at[t]).wait()
        both = peer_gradient_out.at[:, :, 0:wide]
        arrived(both, gossip_send.at[t])
        return carry

    lax.fori_loop(0, steps, drain, 0)
    for k in range(2):
        arrived(peer_numerator_out.at[k], state_send.at[k])
        arrived(peer_numerator_out.at[k], state_recv.at[k])
        arrived(peer_gradient_out.at[k], gossip_recv.at[k])
        arrived(meta.at[k + 1], meta_send.at[k])
        arrived(meta.at[k + 1], meta_recv.at[k])

    step = step_ref[0]
    rate = learning_rate / jnp.sqrt(1.0 + jnp.full((8, LANES), step, jnp.int32).astype(f32) / decay_steps)
    far = jnp.full((8, LANES), step % 2, jnp.int32) == 1
    own_factor = rate * jnp.minimum(1.0, clip_ceiling / jnp.sqrt(square_sum / entry_count + epsilon))
    peer = jnp.where(far, meta[2], meta[1])
    peer_sum = jnp.broadcast_to(peer[0:1], (8, LANES))
    peer_factor = rate * jnp.minimum(1.0, clip_ceiling / jnp.sqrt(peer_sum / entry_count + epsilon))
    mixed_weight = 0.5 * (own_weight + jnp.broadcast_to(peer[1:2], (8, LANES)))
    coefficients_out[0] = own_factor
    coefficients_out[1] = peer_factor
    coefficients_out[2] = mixed_weight


def shards_step(mesh, step_index, hidden, upstream, numerator, push_weight):
    own_hidden, own_upstream, own_state = hidden[0], upstream[0], numerator[0]
    tokens, units = own_hidden.shape
    width = own_upstream.shape[1]
    rows = own_state.shape[0]
    shards = mesh.shape["shard"]
    steps = width // (2 * LANES)
    block = (RING, rows, LANES)
    anywhere = pl.BlockSpec(memory_space=pl.ANY)
    smem = pl.BlockSpec(memory_space=pltpu.SMEM)
    dma = pltpu.SemaphoreType.DMA
    gradient, peer_gradient, peer_numerator, coefficients = pl.pallas_call(
        functools.partial(kernel, float(rows * shards * width)),
        out_shape=(
            jax.ShapeDtypeStruct((rows, width), f32),
            jax.ShapeDtypeStruct((2, rows, width), bf16),
            jax.ShapeDtypeStruct((2, rows, width), bf16),
            jax.ShapeDtypeStruct((3, 8, LANES), f32),
        ),
        in_specs=[smem, smem, anywhere, anywhere, anywhere],
        out_specs=(anywhere, anywhere, anywhere, pl.BlockSpec(memory_space=pltpu.VMEM)),
        scratch_shapes=[
            pltpu.VMEM((tokens, units), bf16),
            pltpu.VMEM((tokens, width), bf16),
            pltpu.VMEM((rows, width), f32),
            pltpu.VMEM((rows, width), bf16),
            pltpu.VMEM((steps, 2, RING, 2) + block, bf16),
            pltpu.VMEM((steps, 2, 2) + block, bf16),
            pltpu.VMEM((steps, 2, 4) + block, bf16),
            pltpu.VMEM((steps, 2) + block, bf16),
            pltpu.VMEM((steps, 2, RING - 1, rows, LANES), bf16),
            pltpu.VMEM((steps, rows, 2 * LANES), f32),
            pltpu.VMEM((steps, rows, 2 * LANES), bf16),
            pltpu.VMEM((8, LANES), f32),
            pltpu.VMEM((shards, LANES), f32),
            pltpu.VMEM((3, 8, LANES), f32),
            dma((7,)), dma((steps,)),
            dma((steps,)), dma((steps, 2, 2)), dma((steps,)), dma((steps, 2)),
            dma((steps,)), dma((steps, 2)), dma((steps,)), dma((steps, 2)),
            dma((steps,)), dma((2,)), dma((2,)), dma((2,)), dma((1,)), dma((1,)), dma((2,)), dma((2,)),
        ],
        compiler_params=pltpu.CompilerParams(
            collective_id=0, has_side_effects=True, vmem_limit_bytes=67_043_328
        ),
        name="reduce_and_gossip",
    )(step_index, push_weight, own_hidden, own_upstream, own_state)
    own_factor, peer_factor, weight = (coefficients[i, 0, 0] for i in range(3))
    far = step_index[0] % 2 == 1
    peer_numerator = jnp.where(far, peer_numerator[1], peer_numerator[0]).astype(f32)
    peer_gradient = jnp.where(far, peer_gradient[1], peer_gradient[0]).astype(f32)
    pushed = own_state - own_factor * gradient
    mixed = 0.5 * (pushed + (peer_numerator - peer_factor * peer_gradient))
    return mixed[None], weight[None], (mixed / weight).astype(bf16)[None]


def solution(mesh):
    placed = (
        P(),
        P("group", "shard", None),
        P("group", "shard", None),
        P("group", "shard", None),
        P("group"),
    )
    return jax.shard_map(
        functools.partial(shards_step, mesh),
        mesh=mesh,
        in_specs=placed,
        out_specs=(P("group", "shard", None), P("group"), P("group", "shard", None)),
        check_vma=False,
    )
```

```python
import functools

import jax
import jax.numpy as jnp
from jax import lax
from jax.experimental import pallas as pl
from jax.experimental.pallas import tpu as pltpu
from jax.sharding import PartitionSpec as P

learning_rate = 0.3
decay_steps = 256.0
clip_ceiling = 1.0
epsilon = 1e-06

MESH = pl.DeviceIdType.MESH
RING = 4
LANES = 128
BANDS = 3
f32 = jnp.float32
bf16 = jnp.bfloat16


def kernel(
    entry_count, ahead,
    step_ref, weight_ref, hidden_hbm, upstream_hbm, numerator_hbm,
    gradient_out, peer_gradient_out, peer_numerator_out, coefficients_out,
    hidden, upstream, numerator, numerator_short, part, transit, final, early_final, across, last,
    gradient, gradient_short, squares, norms, weights,
    load_sem, out_sem, transit_send, transit_recv, final_send, final_recv,
    across_send, across_recv, last_send, last_recv, gossip_send, gossip_recv,
    state_send, state_recv, norm_send, norm_recv, weight_send, weight_recv, token,
    early_transit_send, early_transit_recv, early_final_send, early_final_recv,
):
    units = part.shape[0]
    rows = part.shape[5]
    whole_rows = numerator.shape[0]
    early = units - 1
    quarter = hidden.shape[1] // RING
    group = lax.axis_index("group")
    shard = lax.axis_index("shard")
    groups = lax.axis_size("group")
    shards = lax.axis_size("shard")
    z = shard // (2 * RING)
    y = (shard // 2) % RING
    xh = shard % 2

    def place(kind, first, second, half):
        zz, yy = (first, second) if kind == 0 else (second, first)
        return (group, zz * (2 * RING) + yy * 2 + half)

    def send(src, dst, send_sem, recv_sem, device):
        pltpu.make_async_remote_copy(
            src_ref=src, dst_ref=dst, send_sem=send_sem, recv_sem=recv_sem,
            device_id=device, device_id_type=MESH,
        ).start()

    def arrived(ref, sem):
        pltpu.make_async_copy(ref, ref, sem).wait()

    own = ((z, y), (y, z))
    target = ((group + ahead) % groups, shard)

    def hidden_columns(i):
        block = (z + (2, 1, 3, 0)[i]) % RING if isinstance(i, int) else None
        return pl.ds(pl.multiple_of(block * quarter, LANES), quarter)

    wide = 2 * LANES
    loads = []
    loads.append(pltpu.make_async_copy(upstream_hbm.at[:, 0:wide], upstream.at[:, 0:wide], load_sem.at[4]))
    for i in range(RING):
        loads.append(pltpu.make_async_copy(
            hidden_hbm.at[:, hidden_columns(i)], hidden.at[:, hidden_columns(i)], load_sem.at[i]))
    loads.append(pltpu.make_async_copy(upstream_hbm.at[:, wide:], upstream.at[:, wide:], load_sem.at[5]))
    loads.append(pltpu.make_async_copy(numerator_hbm, numerator, load_sem.at[6]))
    for i in (0, 1, 6, 2, 3, 4, 5):
        loads[i].start()

    barrier = pltpu.get_barrier_semaphore()
    partners = [(group, place(0, (z + k) % RING, y, xh)[1]) for k in range(1, RING)]
    partners += [(group, place(0, z, (y + k) % RING, xh)[1]) for k in range(1, RING)]
    partners += [(group, place(0, z, y, 1 - xh)[1])]
    partners += [((group + k) % groups, shard) for k in range(1, RING)]
    for device in partners:
        pl.semaphore_signal(barrier, inc=1, device_id=device, device_id_type=MESH)
    squares[...] = jnp.zeros_like(squares)
    weights[0] = jnp.full((8, LANES), weight_ref[0], f32)
    loads[0].wait()

    def sum_of(*refs):
        total = refs[0][...].astype(f32)
        for ref in refs[1:]:
            total = total + ref[...].astype(f32)
        return total

    def open_step(t):
        def block(i, carry):
            to = (z + distance_of(i)) % RING

            for j in range(RING):
                @pl.when((t == 0) & (i == j))
                def _(j=j):
                    loads[1 + j].wait()

            multiply(t, to)

            @pl.when((t == 0) & (i == 0))
            def _():
                loads[6].wait()
                numerator_short[...] = numerator[...].astype(bf16)
                pl.semaphore_wait(barrier, len(partners))

            @pl.when(i == 0)
            def _():
                first_sends(t, 0)

            @pl.when(i == 1)
            def _():
                direct_send(t, 0, 1)

            @pl.when(i == 2)
            def _():
                direct_send(t, 0, 3)

            return carry

        lax.fori_loop(0, RING, block, 0)
        first_sends(t, 1)
        direct_send(t, 1, 1)
        direct_send(t, 1, 3)

    def distance_of(i):
        return jnp.where(i == 0, 2, jnp.where(i == 1, 1, jnp.where(i == 2, 3, 0)))

    def multiply(t, to):
        product = lax.dot_general(
            hidden[:, pl.ds(pl.multiple_of(to * quarter, LANES), quarter)],
            upstream[:, pl.ds(pl.multiple_of(t * wide, wide), wide)],
            (((0,), (0,)), ((), ())),
            preferred_element_type=f32,
        )
        for b in range(RING):
            for h in range(2):
                at = (b * 2 + h) * rows
                part[t, 0, to, h, b] = product[at:at + rows, :LANES].astype(bf16)
                part[t, 1, b, h, to] = product[at:at + rows, LANES:].astype(bf16)

    def early_begin():
        loads[5].wait()

        def block(i, carry):
            multiply(early, (z + distance_of(i)) % RING)
            return carry

        lax.fori_loop(0, RING, block, 0)
        for kind in range(2):
            a, b = own[kind]
            send(part.at[early, kind, :, 1 - xh], final.at[early, kind], final_send.at[early],
                 final_recv.at[early, kind], place(kind, a, b, 1 - xh))
        send(weights.at[0], weights.at[1], weight_send, weight_recv, target)

    def early_sum():
        for kind in range(2):
            arrived(final.at[early, kind], final_recv.at[early, kind])
            for c in range(RING):
                part[early, kind, c, xh] = sum_of(part.at[early, kind, c, xh], final.at[early, kind, c]).astype(bf16)

    def early_sends():
        for kind in range(2):
            a, b = own[kind]
            to = (a + 2) % RING
            for h, hop in ((0, 3), (1, 1)):
                send(part.at[early, kind, to, xh, 2 * h:2 * h + 2], transit.at[early, kind, h, 0:2], early_transit_send,
                     early_transit_recv.at[kind, h], place(kind, (a + hop) % RING, b, xh))
        for kind in range(2):
            a, b = own[kind]
            for h, hop in ((0, 1), (1, 3)):
                to = (a + hop) % RING
                send(part.at[early, kind, to, xh, 2 * h:2 * h + 2], early_final.at[kind, h], early_final_send,
                     early_final_recv.at[kind], place(kind, to, b, xh))

    def early_relay():
        for kind in range(2):
            a, b = own[kind]
            for h, hop in ((0, 3), (1, 1)):
                to = (a + hop) % RING
                mine = part.at[early, kind, to, xh, 2 * h:2 * h + 2]
                arrived(transit.at[early, kind, h, 0:2], early_transit_recv.at[kind, h])
                mine[...] = sum_of(mine, transit.at[early, kind, h, 0:2]).astype(bf16)
                send(mine, early_final.at[kind, 2 + h], early_final_send,
                     early_final_recv.at[kind], place(kind, to, b, xh))

    def early_last():
        for kind in range(2):
            a, b = own[kind]
            arrived(early_final.at[kind], early_final_recv.at[kind])
            for h in range(2):
                mine = part.at[early, kind, a, xh, 2 * h:2 * h + 2]
                mine[...] = sum_of(mine, early_final.at[kind, h], early_final.at[kind, 2 + h]).astype(bf16)
            last_sends(early, kind)

    def first_sends(t, kind):
        a, b = own[kind]
        to = (a + 2) % RING
        for h, hop in ((0, 3), (1, 1)):
            send(part.at[t, kind, to, h], transit.at[t, kind, h], transit_send.at[t],
                 transit_recv.at[t, kind, h], place(kind, (a + hop) % RING, b, xh))

    def direct_send(t, kind, hop):
        a, b = own[kind]
        to = (a + hop) % RING
        h = 0 if hop == 1 else 1
        send(part.at[t, kind, to, h], final.at[t, kind, h], final_send.at[t],
             final_recv.at[t, kind], place(kind, to, b, xh))

    def relay_step(t):
        for kind in range(2):
            a, b = own[kind]
            for h, hop in ((0, 3), (1, 1)):
                to = (a + hop) % RING
                arrived(transit.at[t, kind, h], transit_recv.at[t, kind, h])
                part[t, kind, to, h] = sum_of(part.at[t, kind, to, h], transit.at[t, kind, h]).astype(bf16)
                send(part.at[t, kind, to, h], final.at[t, kind, 2 + h], final_send.at[t],
                     final_recv.at[t, kind], place(kind, to, b, xh))

    def across_step(t):
        for kind in range(2):
            a, b = own[kind]
            arrived(final.at[t, kind], final_recv.at[t, kind])
            for h in range(2):
                part[t, kind, a, h] = sum_of(
                    part.at[t, kind, a, h], final.at[t, kind, h], final.at[t, kind, 2 + h]).astype(bf16)
            send(part.at[t, kind, a, 1 - xh], across.at[t, kind], across_send.at[t],
                 across_recv.at[t, kind], place(kind, a, b, 1 - xh))

    def last_step(t):
        for kind in range(2):
            a, b = own[kind]
            arrived(across.at[t, kind], across_recv.at[t, kind])
            part[t, kind, a, xh] = sum_of(part.at[t, kind, a, xh], across.at[t, kind]).astype(bf16)
            last_sends(t, kind)

    def last_sends(t, kind):
        a, b = own[kind]
        for hop in (2, 1, 3):
            to = (b + hop) % RING
            send(part.at[t, kind, a, xh, to], last.at[t, kind, hop - 1], last_send.at[t],
                 last_recv.at[t, kind], place(kind, a, to, xh))

    def state_chunk(t):
        columns = pl.ds(pl.multiple_of(t * wide, wide), wide)
        send(numerator_short.at[:, columns], peer_numerator_out.at[:, columns], state_send, state_recv, target)

    def tell_norms():
        norms[0, 0:1] = jnp.sum(squares[...], axis=0, keepdims=True)
        pl.semaphore_wait(token, 1)

        def tell(k, carry):
            other = (shard + k) % shards

            @pl.when(k > 0)
            def _():
                send(norms.at[0, 0:1], norms.at[0, pl.ds(k, 1)], norm_send.at[0], norm_recv.at[0], (group, other))

            send(norms.at[0, 0:1], norms.at[1, pl.ds(k, 1)], norm_send.at[1], norm_recv.at[1],
                 ((group + ahead) % groups, other))
            return carry

        lax.fori_loop(0, shards, tell, 0)

    def close_step(t):
        for kind in range(2):
            a, b = own[kind]
            arrived(last.at[t, kind], last_recv.at[t, kind])
            total = sum_of(part.at[t, kind, a, xh, b], last.at[t, kind, 0], last.at[t, kind, 1], last.at[t, kind, 2])
            at = slice(kind * LANES, (kind + 1) * LANES)
            gradient[t, :, at] = total
            gradient_short[t, :, at] = total.astype(bf16)
            squares[...] += jnp.sum((total * total).reshape(rows // 8, 8, LANES), axis=0)
        columns = pl.ds(pl.multiple_of(t * wide, wide), wide)

        @pl.when(t == units - 1)
        def _():
            tell_norms()

        send(gradient_short.at[t], peer_gradient_out.at[:, columns], gossip_send.at[t], gossip_recv, target)
        pltpu.make_async_copy(gradient.at[t], gradient_out.at[:, columns], out_sem.at[t]).start()

        @pl.when(t == 0)
        def _():
            source = ((group + groups - ahead) % groups, shard)
            pl.semaphore_signal(token, inc=1, device_id=source, device_id_type=MESH)

    def turn(t, carry):
        schedule = (
            (t < early, lambda: open_step(t)),
            (t == 0, early_begin),
            ((t >= 1) & (t < early + 1), lambda: relay_step(t - 1)),
            (t == early - 2, early_sum),
            (t == early, early_sends),
            ((t >= 1) & (t < units + 1), lambda: state_chunk(t - 1)),
            ((t >= 2) & (t < early + 2), lambda: across_step(t - 2)),
            (t == early + 1, early_relay),
            (t == early + 2, early_last),
            ((t >= 4) & (t < early + 4), lambda: last_step(t - 4)),
            (t >= 6, lambda: close_step(t - 6)),
        )
        for condition, stage in schedule:
            pl.when(condition)(stage)
        return carry

    lax.fori_loop(0, units + 6, turn, 0)

    def drain(t, carry):
        @pl.when(t < early)
        def _():
            arrived(transit.at[t], transit_send.at[t])
            arrived(across.at[t], across_send.at[t])

        arrived(final.at[t], final_send.at[t])
        arrived(last.at[t], last_send.at[t])
        pltpu.make_async_copy(gradient.at[t], gradient_out.at[:, 0:wide], out_sem.at[t]).wait()
        arrived(gradient_short.at[t], gossip_send.at[t])
        return carry

    lax.fori_loop(0, units, drain, 0)
    arrived(transit.at[early, :, :, 0:2], early_transit_send)
    arrived(early_final, early_final_send)
    for ref, sent, received in (
        (peer_numerator_out, state_send, state_recv), (weights.at[1], weight_send, weight_recv)):
        arrived(ref, sent)
        arrived(ref, received)
    arrived(peer_gradient_out, gossip_recv)

    rate = learning_rate / jnp.sqrt(1.0 + jnp.full((8, LANES), step_ref[0], jnp.int32).astype(f32) / decay_steps)

    def factor(of):
        square_sum = jnp.sum(norms[of], keepdims=True)
        return rate * jnp.minimum(1.0, clip_ceiling / jnp.sqrt(square_sum / entry_count + epsilon))

    arrived(norms.at[0, 1:shards], norm_recv.at[0])
    arrived(norms.at[1], norm_recv.at[1])
    coefficients_out[0] = factor(0)
    coefficients_out[1] = factor(1)
    coefficients_out[2] = 0.5 * (weights[0] + weights[1])
    arrived(norms.at[0, 1:shards], norm_send.at[0])
    arrived(norms.at[1], norm_send.at[1])


def mix(coefficients, numerator, gradient, peer_numerator, peer_gradient, mixed_out, weight_out, params_out):
    own_factor = coefficients[0, 0:1, 0:1]
    peer_factor = coefficients[1, 0:1, 0:1]
    weight = coefficients[2, 0:1, 0:1]
    pushed = numerator[...] - own_factor * gradient[...]
    peer = peer_numerator[...].astype(f32) - peer_factor * peer_gradient[...].astype(f32)
    mixed = 0.5 * (pushed + peer)
    mixed_out[...] = mixed
    params_out[...] = (mixed / weight).astype(bf16)
    weight_out[...] = coefficients[2, 0, 0:1]


def gossip_step(ahead, mesh, step_index, own_hidden, own_upstream, own_state, push_weight):
    tokens, units = own_hidden.shape
    width = own_upstream.shape[1]
    whole_rows = own_state.shape[0]
    shards = mesh.shape["shard"]
    rows = whole_rows
    parts = width // (2 * LANES)
    block = (RING, rows, LANES)
    anywhere = pl.BlockSpec(memory_space=pl.ANY)
    smem = pl.BlockSpec(memory_space=pltpu.SMEM)
    dma = pltpu.SemaphoreType.DMA
    gradient, peer_gradient, peer_numerator, coefficients = pl.pallas_call(
        functools.partial(kernel, float(whole_rows * shards * width), ahead),
        out_shape=(
            jax.ShapeDtypeStruct((whole_rows, width), f32),
            jax.ShapeDtypeStruct((whole_rows, width), bf16),
            jax.ShapeDtypeStruct((whole_rows, width), bf16),
            jax.ShapeDtypeStruct((3, 8, LANES), f32),
        ),
        in_specs=[smem, smem, anywhere, anywhere, anywhere],
        out_specs=(anywhere, anywhere, anywhere, pl.BlockSpec(memory_space=pltpu.VMEM)),
        scratch_shapes=[
            pltpu.VMEM((tokens, units), bf16),
            pltpu.VMEM((tokens, width), bf16),
            pltpu.VMEM((whole_rows, width), f32),
            pltpu.VMEM((whole_rows, width), bf16),
            pltpu.VMEM((parts, 2, RING, 2) + block, bf16),
            pltpu.VMEM((parts, 2, 2) + block, bf16),
            pltpu.VMEM((parts, 2, 4) + block, bf16),
            pltpu.VMEM((2, 4, 2, rows, LANES), bf16),
            pltpu.VMEM((parts - 1, 2) + block, bf16),
            pltpu.VMEM((parts, 2, RING - 1, rows, LANES), bf16),
            pltpu.VMEM((parts, rows, 2 * LANES), f32),
            pltpu.VMEM((parts, rows, 2 * LANES), bf16),
            pltpu.VMEM((8, LANES), f32),
            pltpu.VMEM((2, shards, LANES), f32),
            pltpu.VMEM((2, 8, LANES), f32),
            dma((7,)), dma((parts,)),
            dma((parts,)), dma((parts, 2, 2)), dma((parts,)), dma((parts, 2)),
            dma((parts,)), dma((parts, 2)), dma((parts,)), dma((parts, 2)),
            dma((parts,)), dma, dma, dma, dma((2,)), dma((2,)), dma, dma,
            pltpu.SemaphoreType.REGULAR,
            dma, dma((2, 2)), dma, dma((2,)),
        ],
        compiler_params=pltpu.CompilerParams(
            collective_id=ahead, has_side_effects=True, vmem_limit_bytes=67_043_328
        ),
        name=f"reduce_and_gossip_{ahead}",
    )(step_index, push_weight, own_hidden, own_upstream, own_state)

    band = pl.BlockSpec((whole_rows // BANDS, width), lambda i: (i, 0))
    mixed, weight, params = pl.pallas_call(
        mix,
        out_shape=(
            jax.ShapeDtypeStruct((whole_rows, width), f32),
            jax.ShapeDtypeStruct((1,), f32),
            jax.ShapeDtypeStruct((whole_rows, width), bf16),
        ),
        grid=(BANDS,),
        in_specs=[pl.BlockSpec((3, 8, LANES), lambda i: (0, 0, 0)), band, band, band, band],
        out_specs=(band, pl.BlockSpec((1,), lambda i: (0,)), band),
        name=f"mix_{ahead}",
    )(coefficients, own_state, gradient, peer_numerator, peer_gradient)
    return mixed, weight, params


def shards_step(mesh, step_index, hidden, upstream, numerator, push_weight):
    branches = [functools.partial(gossip_step, 1 << bit, mesh) for bit in range(2)]
    mixed, weight, params = lax.switch(
        step_index[0] & 1, branches, step_index, hidden[0], upstream[0], numerator[0], push_weight)
    return mixed[None], weight, params[None]


def solution(mesh):
    placed = (
        P(),
        P("group", "shard", None),
        P("group", "shard", None),
        P("group", "shard", None),
        P("group"),
    )
    return jax.shard_map(
        functools.partial(shards_step, mesh),
        mesh=mesh,
        in_specs=placed,
        out_specs=(P("group", "shard", None), P("group"), P("group", "shard", None)),
        check_vma=False,
    )
```

```python
import functools

import jax
import jax.numpy as jnp
from jax import lax
from jax.experimental import pallas as pl
from jax.experimental.pallas import tpu as pltpu
from jax.sharding import PartitionSpec as P

learning_rate = 0.3
decay_steps = 256.0
clip_ceiling = 1.0
epsilon = 1e-06

MESH = pl.DeviceIdType.MESH
RING = 4
LANES = 128
BANDS = 1
f32 = jnp.float32
bf16 = jnp.bfloat16


def kernel(
    entry_count, ahead,
    step_ref, weight_ref, hidden_hbm, upstream_hbm, numerator_hbm,
    gradient_out, peer_gradient_out, peer_numerator_out, coefficients_out,
    hidden, upstream, numerator, numerator_short, part, transit, final, early_final, across, last,
    gradient, gradient_short, squares, norms, weights,
    load_sem, out_sem, transit_send, transit_recv, final_send, final_recv,
    across_send, across_recv, last_send, last_recv, gossip_send, gossip_recv,
    state_send, state_recv, norm_send, norm_recv, weight_send, weight_recv, token,
    early_transit_send, early_transit_recv, early_final_send, early_final_recv,
):
    units = part.shape[0]
    rows = part.shape[5]
    whole_rows = numerator.shape[0]
    early = units - 1
    quarter = hidden.shape[1] // RING
    group = lax.axis_index("group")
    shard = lax.axis_index("shard")
    groups = lax.axis_size("group")
    shards = lax.axis_size("shard")
    z = shard // (2 * RING)
    y = (shard // 2) % RING
    xh = shard % 2

    def place(kind, first, second, half):
        zz, yy = (first, second) if kind == 0 else (second, first)
        return (group, zz * (2 * RING) + yy * 2 + half)

    def send(src, dst, send_sem, recv_sem, device):
        pltpu.make_async_remote_copy(
            src_ref=src, dst_ref=dst, send_sem=send_sem, recv_sem=recv_sem,
            device_id=device, device_id_type=MESH,
        ).start()

    def arrived(ref, sem):
        pltpu.make_async_copy(ref, ref, sem).wait()

    own = ((z, y), (y, z))
    target = ((group + ahead) % groups, shard)

    def hidden_columns(i):
        block = (z + (2, 1, 3, 0)[i]) % RING if isinstance(i, int) else None
        return pl.ds(pl.multiple_of(block * quarter, LANES), quarter)

    wide = 2 * LANES
    loads = []
    loads.append(pltpu.make_async_copy(upstream_hbm.at[:, 0:wide], upstream.at[:, 0:wide], load_sem.at[4]))
    for i in range(RING):
        loads.append(pltpu.make_async_copy(
            hidden_hbm.at[:, hidden_columns(i)], hidden.at[:, hidden_columns(i)], load_sem.at[i]))
    loads.append(pltpu.make_async_copy(upstream_hbm.at[:, wide:], upstream.at[:, wide:], load_sem.at[5]))
    loads.append(pltpu.make_async_copy(numerator_hbm, numerator, load_sem.at[6]))
    for i in (0, 1, 6, 2, 3, 4, 5):
        loads[i].start()

    barrier = pltpu.get_barrier_semaphore()
    partners = [(group, place(0, (z + k) % RING, y, xh)[1]) for k in range(1, RING)]
    partners += [(group, place(0, z, (y + k) % RING, xh)[1]) for k in range(1, RING)]
    partners += [(group, place(0, z, y, 1 - xh)[1])]
    partners += [((group + k) % groups, shard) for k in range(1, RING)]
    for device in partners:
        pl.semaphore_signal(barrier, inc=1, device_id=device, device_id_type=MESH)
    squares[...] = jnp.zeros_like(squares)
    weights[0] = jnp.full((8, LANES), weight_ref[0], f32)
    loads[0].wait()

    def sum_of(*refs):
        total = refs[0][...].astype(f32)
        for ref in refs[1:]:
            total = total + ref[...].astype(f32)
        return total

    def open_step(t):
        def block(i, carry):
            to = (z + distance_of(i)) % RING

            for j in range(RING):
                @pl.when((t == 0) & (i == j))
                def _(j=j):
                    loads[1 + j].wait()

            multiply(t, to)

            @pl.when((t == 0) & (i == 0))
            def _():
                loads[6].wait()
                numerator_short[...] = numerator[...].astype(bf16)
                pl.semaphore_wait(barrier, len(partners))

            @pl.when(i == 0)
            def _():
                first_sends(t, 0)

            @pl.when(i == 1)
            def _():
                direct_send(t, 0, 1)

            @pl.when(i == 2)
            def _():
                direct_send(t, 0, 3)

            return carry

        lax.fori_loop(0, RING, block, 0)
        first_sends(t, 1)
        direct_send(t, 1, 1)
        direct_send(t, 1, 3)

    def distance_of(i):
        return jnp.where(i == 0, 2, jnp.where(i == 1, 1, jnp.where(i == 2, 3, 0)))

    def multiply(t, to):
        product = lax.dot_general(
            hidden[:, pl.ds(pl.multiple_of(to * quarter, LANES), quarter)],
            upstream[:, pl.ds(pl.multiple_of(t * wide, wide), wide)],
            (((0,), (0,)), ((), ())),
            preferred_element_type=f32,
        )
        for b in range(RING):
            for h in range(2):
                at = (b * 2 + h) * rows
                part[t, 0, to, h, b] = product[at:at + rows, :LANES].astype(bf16)
                part[t, 1, b, h, to] = product[at:at + rows, LANES:].astype(bf16)

    def early_begin():
        loads[5].wait()

        def block(i, carry):
            multiply(early, (z + distance_of(i)) % RING)
            return carry

        lax.fori_loop(0, RING, block, 0)
        for kind in range(2):
            a, b = own[kind]
            send(part.at[early, kind, :, 1 - xh], final.at[early, kind], final_send.at[early],
                 final_recv.at[early, kind], place(kind, a, b, 1 - xh))
        send(weights.at[0], weights.at[1], weight_send, weight_recv, target)

    def early_sum():
        for kind in range(2):
            arrived(final.at[early, kind], final_recv.at[early, kind])
            for c in range(RING):
                part[early, kind, c, xh] = sum_of(part.at[early, kind, c, xh], final.at[early, kind, c]).astype(bf16)

    def early_sends():
        for kind in range(2):
            a, b = own[kind]
            to = (a + 2) % RING
            for h, hop in ((0, 3), (1, 1)):
                send(part.at[early, kind, to, xh, 2 * h:2 * h + 2], transit.at[early, kind, h, 0:2], early_transit_send,
                     early_transit_recv.at[kind, h], place(kind, (a + hop) % RING, b, xh))
        for kind in range(2):
            a, b = own[kind]
            for h, hop in ((0, 1), (1, 3)):
                to = (a + hop) % RING
                send(part.at[early, kind, to, xh, 2 * h:2 * h + 2], early_final.at[kind, h], early_final_send,
                     early_final_recv.at[kind], place(kind, to, b, xh))

    def early_relay():
        for kind in range(2):
            a, b = own[kind]
            for h, hop in ((0, 3), (1, 1)):
                to = (a + hop) % RING
                mine = part.at[early, kind, to, xh, 2 * h:2 * h + 2]
                arrived(transit.at[early, kind, h, 0:2], early_transit_recv.at[kind, h])
                mine[...] = sum_of(mine, transit.at[early, kind, h, 0:2]).astype(bf16)
                send(mine, early_final.at[kind, 2 + h], early_final_send,
                     early_final_recv.at[kind], place(kind, to, b, xh))

    def early_last():
        for kind in range(2):
            a, b = own[kind]
            arrived(early_final.at[kind], early_final_recv.at[kind])
            for h in range(2):
                mine = part.at[early, kind, a, xh, 2 * h:2 * h + 2]
                mine[...] = sum_of(mine, early_final.at[kind, h], early_final.at[kind, 2 + h]).astype(bf16)
            last_sends(early, kind)

    def first_sends(t, kind):
        a, b = own[kind]
        to = (a + 2) % RING
        for h, hop in ((0, 3), (1, 1)):
            send(part.at[t, kind, to, h], transit.at[t, kind, h], transit_send.at[t],
                 transit_recv.at[t, kind, h], place(kind, (a + hop) % RING, b, xh))

    def direct_send(t, kind, hop):
        a, b = own[kind]
        to = (a + hop) % RING
        h = 0 if hop == 1 else 1
        send(part.at[t, kind, to, h], final.at[t, kind, h], final_send.at[t],
             final_recv.at[t, kind], place(kind, to, b, xh))

    def relay_step(t):
        for kind in range(2):
            a, b = own[kind]
            for h, hop in ((0, 3), (1, 1)):
                to = (a + hop) % RING
                arrived(transit.at[t, kind, h], transit_recv.at[t, kind, h])
                part[t, kind, to, h] = sum_of(part.at[t, kind, to, h], transit.at[t, kind, h]).astype(bf16)
                send(part.at[t, kind, to, h], final.at[t, kind, 2 + h], final_send.at[t],
                     final_recv.at[t, kind], place(kind, to, b, xh))

    def across_step(t):
        for kind in range(2):
            a, b = own[kind]
            arrived(final.at[t, kind], final_recv.at[t, kind])
            for h in range(2):
                part[t, kind, a, h] = sum_of(
                    part.at[t, kind, a, h], final.at[t, kind, h], final.at[t, kind, 2 + h]).astype(bf16)
            send(part.at[t, kind, a, 1 - xh], across.at[t, kind], across_send.at[t],
                 across_recv.at[t, kind], place(kind, a, b, 1 - xh))

    def last_step(t):
        for kind in range(2):
            a, b = own[kind]
            arrived(across.at[t, kind], across_recv.at[t, kind])
            part[t, kind, a, xh] = sum_of(part.at[t, kind, a, xh], across.at[t, kind]).astype(bf16)
            last_sends(t, kind)

    def last_sends(t, kind):
        a, b = own[kind]
        for hop in (2, 1, 3):
            to = (b + hop) % RING
            send(part.at[t, kind, a, xh, to], last.at[t, kind, hop - 1], last_send.at[t],
                 last_recv.at[t, kind], place(kind, a, to, xh))

    def state_chunk(t):
        columns = pl.ds(pl.multiple_of(t * wide, wide), wide)
        send(numerator_short.at[:, columns], peer_numerator_out.at[:, columns], state_send, state_recv, target)

    def tell_norms():
        norms[0, 0:1] = jnp.sum(squares[...], axis=0, keepdims=True)
        pl.semaphore_wait(token, 1)

        def tell(k, carry):
            other = (shard + k) % shards

            @pl.when(k > 0)
            def _():
                send(norms.at[0, 0:1], norms.at[0, pl.ds(k, 1)], norm_send.at[0], norm_recv.at[0], (group, other))

            send(norms.at[0, 0:1], norms.at[1, pl.ds(k, 1)], norm_send.at[1], norm_recv.at[1],
                 ((group + ahead) % groups, other))
            return carry

        lax.fori_loop(0, shards, tell, 0)

    def close_step(t):
        for kind in range(2):
            a, b = own[kind]
            arrived(last.at[t, kind], last_recv.at[t, kind])
            total = sum_of(part.at[t, kind, a, xh, b], last.at[t, kind, 0], last.at[t, kind, 1], last.at[t, kind, 2])
            at = slice(kind * LANES, (kind + 1) * LANES)
            gradient[t, :, at] = total
            gradient_short[t, :, at] = total.astype(bf16)
            squares[...] += jnp.sum((total * total).reshape(rows // 8, 8, LANES), axis=0)
        columns = pl.ds(pl.multiple_of(t * wide, wide), wide)

        @pl.when(t == units - 1)
        def _():
            tell_norms()

        send(gradient_short.at[t], peer_gradient_out.at[:, columns], gossip_send.at[t], gossip_recv, target)
        pltpu.make_async_copy(gradient.at[t], gradient_out.at[:, columns], out_sem.at[t]).start()

        @pl.when(t == 0)
        def _():
            source = ((group + groups - ahead) % groups, shard)
            pl.semaphore_signal(token, inc=1, device_id=source, device_id_type=MESH)

    def turn(t, carry):
        schedule = (
            (t < early, lambda: open_step(t)),
            (t == 0, early_begin),
            ((t >= 1) & (t < early + 1), lambda: relay_step(t - 1)),
            (t == early - 2, early_sum),
            (t == early, early_sends),
            ((t >= 1) & (t < units + 1), lambda: state_chunk(t - 1)),
            ((t >= 2) & (t < early + 2), lambda: across_step(t - 2)),
            (t == early + 1, early_relay),
            (t == early + 2, early_last),
            ((t >= 5) & (t < early + 5), lambda: last_step(t - 5)),
            (t >= 7, lambda: close_step(t - 7)),
        )
        for condition, stage in schedule:
            pl.when(condition)(stage)
        return carry

    lax.fori_loop(0, units + 7, turn, 0)

    def drain(t, carry):
        @pl.when(t < early)
        def _():
            arrived(transit.at[t], transit_send.at[t])
            arrived(across.at[t], across_send.at[t])

        arrived(final.at[t], final_send.at[t])
        arrived(last.at[t], last_send.at[t])
        pltpu.make_async_copy(gradient.at[t], gradient_out.at[:, 0:wide], out_sem.at[t]).wait()
        arrived(gradient_short.at[t], gossip_send.at[t])
        return carry

    lax.fori_loop(0, units, drain, 0)
    arrived(transit.at[early, :, :, 0:2], early_transit_send)
    arrived(early_final, early_final_send)
    for ref, sent, received in (
        (peer_numerator_out, state_send, state_recv), (weights.at[1], weight_send, weight_recv)):
        arrived(ref, sent)
        arrived(ref, received)
    arrived(peer_gradient_out, gossip_recv)

    rate = learning_rate / jnp.sqrt(1.0 + jnp.full((8, LANES), step_ref[0], jnp.int32).astype(f32) / decay_steps)

    def factor(of):
        square_sum = jnp.sum(norms[of], keepdims=True)
        return rate * jnp.minimum(1.0, clip_ceiling / jnp.sqrt(square_sum / entry_count + epsilon))

    arrived(norms.at[0, 1:shards], norm_recv.at[0])
    arrived(norms.at[1], norm_recv.at[1])
    coefficients_out[0] = factor(0)
    coefficients_out[1] = factor(1)
    coefficients_out[2] = 0.5 * (weights[0] + weights[1])
    arrived(norms.at[0, 1:shards], norm_send.at[0])
    arrived(norms.at[1], norm_send.at[1])


def mix(coefficients, numerator, gradient, peer_numerator, peer_gradient, mixed_out, weight_out, params_out):
    own_factor = coefficients[0, 0:1, 0:1]
    peer_factor = coefficients[1, 0:1, 0:1]
    weight = coefficients[2, 0:1, 0:1]
    pushed = numerator[...] - own_factor * gradient[...]
    peer = peer_numerator[...].astype(f32) - peer_factor * peer_gradient[...].astype(f32)
    mixed = 0.5 * (pushed + peer)
    mixed_out[...] = mixed
    params_out[...] = (mixed / weight).astype(bf16)
    weight_out[...] = coefficients[2, 0, 0:1]


def gossip_step(ahead, mesh, step_index, own_hidden, own_upstream, own_state, push_weight):
    tokens, units = own_hidden.shape
    width = own_upstream.shape[1]
    whole_rows = own_state.shape[0]
    shards = mesh.shape["shard"]
    rows = whole_rows
    parts = width // (2 * LANES)
    block = (RING, rows, LANES)
    anywhere = pl.BlockSpec(memory_space=pl.ANY)
    smem = pl.BlockSpec(memory_space=pltpu.SMEM)
    dma = pltpu.SemaphoreType.DMA
    gradient, peer_gradient, peer_numerator, coefficients = pl.pallas_call(
        functools.partial(kernel, float(whole_rows * shards * width), ahead),
        out_shape=(
            jax.ShapeDtypeStruct((whole_rows, width), f32),
            jax.ShapeDtypeStruct((whole_rows, width), bf16),
            jax.ShapeDtypeStruct((whole_rows, width), bf16),
            jax.ShapeDtypeStruct((3, 8, LANES), f32),
        ),
        in_specs=[smem, smem, anywhere, anywhere, anywhere],
        out_specs=(anywhere, anywhere, anywhere, pl.BlockSpec(memory_space=pltpu.VMEM)),
        scratch_shapes=[
            pltpu.VMEM((tokens, units), bf16),
            pltpu.VMEM((tokens, width), bf16),
            pltpu.VMEM((whole_rows, width), f32),
            pltpu.VMEM((whole_rows, width), bf16),
            pltpu.VMEM((parts, 2, RING, 2) + block, bf16),
            pltpu.VMEM((parts, 2, 2) + block, bf16),
            pltpu.VMEM((parts, 2, 4) + block, bf16),
            pltpu.VMEM((2, 4, 2, rows, LANES), bf16),
            pltpu.VMEM((parts - 1, 2) + block, bf16),
            pltpu.VMEM((parts, 2, RING - 1, rows, LANES), bf16),
            pltpu.VMEM((parts, rows, 2 * LANES), f32),
            pltpu.VMEM((parts, rows, 2 * LANES), bf16),
            pltpu.VMEM((8, LANES), f32),
            pltpu.VMEM((2, shards, LANES), f32),
            pltpu.VMEM((2, 8, LANES), f32),
            dma((7,)), dma((parts,)),
            dma((parts,)), dma((parts, 2, 2)), dma((parts,)), dma((parts, 2)),
            dma((parts,)), dma((parts, 2)), dma((parts,)), dma((parts, 2)),
            dma((parts,)), dma, dma, dma, dma((2,)), dma((2,)), dma, dma,
            pltpu.SemaphoreType.REGULAR,
            dma, dma((2, 2)), dma, dma((2,)),
        ],
        compiler_params=pltpu.CompilerParams(
            collective_id=ahead, has_side_effects=True, vmem_limit_bytes=67_043_328
        ),
        name=f"reduce_and_gossip_{ahead}",
    )(step_index, push_weight, own_hidden, own_upstream, own_state)

    band = pl.BlockSpec((whole_rows // BANDS, width), lambda i: (i, 0))
    mixed, weight, params = pl.pallas_call(
        mix,
        out_shape=(
            jax.ShapeDtypeStruct((whole_rows, width), f32),
            jax.ShapeDtypeStruct((1,), f32),
            jax.ShapeDtypeStruct((whole_rows, width), bf16),
        ),
        grid=(BANDS,),
        in_specs=[pl.BlockSpec((3, 8, LANES), lambda i: (0, 0, 0)), band, band, band, band],
        out_specs=(band, pl.BlockSpec((1,), lambda i: (0,)), band),
        name=f"mix_{ahead}",
    )(coefficients, own_state, gradient, peer_numerator, peer_gradient)
    return mixed, weight, params


def shards_step(mesh, step_index, hidden, upstream, numerator, push_weight):
    branches = [functools.partial(gossip_step, 1 << bit, mesh) for bit in range(2)]
    mixed, weight, params = lax.switch(
        step_index[0] & 1, branches, step_index, hidden[0], upstream[0], numerator[0], push_weight)
    return mixed[None], weight, params[None]


def solution(mesh):
    placed = (
        P(),
        P("group", "shard", None),
        P("group", "shard", None),
        P("group", "shard", None),
        P("group"),
    )
    return jax.shard_map(
        functools.partial(shards_step, mesh),
        mesh=mesh,
        in_specs=placed,
        out_specs=(P("group", "shard", None), P("group"), P("group", "shard", None)),
        check_vma=False,
    )
```
